128 devices in a mesh: batch: 8 (over z, core), seq: 16 (over x, y).
Axes of the slice: x: 4, y: 4, z: 4, core: 2. Of those that a mesh axis runs over, the one named last changes fastest.
Arguments:
- queries: bfloat16 [65536, 8, 256], P(('batch', 'seq')), parts along dimension 0, may hold values from -400 to 400
- key_heads: bfloat16 [65536, 4, 256], P(('batch', 'seq')), parts along dimension 0, may hold values from -16 to 16
- projected_value_heads: bfloat16 [65536, 4, 256], P(('batch', 'seq')), parts along dimension 0, may hold values from -6 to 6
- lengths: int32 [8], P('batch'), parts along dimension 0, may hold values from 7681 to 8192
Outputs:
- attended: bfloat16 [65536, 8, 256], P(('batch', 'seq')), parts along dimension 0
The draws below stay inside these ranges and needn't reach their ends.
There are 8 independent parts, one for each index of `batch`. The reference program is written for one: setup_inputs(seed, part) draws one part's arguments, and reference() takes and returns one part's arrays. A program takes and returns all parts, laid end to end along the dimension named above; each array names one. Nothing has to cross between parts.
All inputs are finite; a program needn't handle non-finite values.
Results may differ from the reference program's by a relative error of at most 0.0033.
Values may be sent and summed in bfloat16 or wider, within the bound.
A program may use at most 192 MiB of HBM per device.

```python
import math
import jax
import jax.numpy as jnp
from jax import lax

QUERY_HEADS = 8
KEY_VALUE_HEADS = 4
HEAD_SIZE = 256
WINDOW = 4096
SINKS = 4
TOK_DEV = 512
ROW_LENGTH = 8192


def joint_draw(key):
    base = jax.random.fold_in(key, 7919)
    leading_key = jax.random.fold_in(base, 0)
    third_key = jax.random.fold_in(base, 2)
    key_value_pairs = jnp.clip(jax.random.normal(leading_key, (ROW_LENGTH, KEY_VALUE_HEADS, HEAD_SIZE), jnp.float32), -6.0, 6.0)
    query_values = 2.5 * jnp.clip(jax.random.normal(third_key, (ROW_LENGTH, QUERY_HEADS, HEAD_SIZE), jnp.float32), -6.0, 6.0)
    sink_boost = jnp.where(jnp.arange(ROW_LENGTH)[:, None, None] < SINKS, 2.0, 1.0)
    key_value_pairs = key_value_pairs * sink_boost
    return (jnp.clip(query_values, -400.0, 400.0), jnp.clip(key_value_pairs, -16.0, 16.0))


def draw_queries(key, part):
    return joint_draw(key)[0].astype(jnp.bfloat16)


def draw_key_heads(key, part):
    return joint_draw(key)[1].astype(jnp.bfloat16)


def steps_of(stream_key, shape, cuts, smallest, top_value):
    def one(position, shards_of):
        steps = jax.random.uniform(jax.random.fold_in(jax.random.fold_in(stream_key, 6), position), (shards_of,), jnp.float32, smallest / len(cuts), top_value / len(cuts))
        return jnp.repeat(jnp.exp(steps), shape[position] // shards_of).reshape((-1,) + (1,) * (len(shape) - position - 1))

    factor_of = one(*cuts[0])
    for cut in cuts[1:]:
        factor_of = factor_of * one(*cut)
    return factor_of


def scatter_about(stream_key, shape, width, most, cuts=(), kind=jnp.bfloat16):
    values = width * jax.random.normal(stream_key, shape, jnp.float32)
    if cuts:
        values = values * steps_of(stream_key, shape, cuts, -0.22, 0.18)
    return jnp.clip(values, -most, most).astype(kind)


def setup_inputs(seed: int = 0, part: int = 0) -> dict:
    streams_of = jax.random.split(jax.random.key(seed), 5)
    part_splits = jax.random.split(jax.random.fold_in(streams_of[4], part), 5)
    queries = draw_queries(jax.random.fold_in(jax.random.fold_in(streams_of[4], part), 71), part)
    key_heads = draw_key_heads(jax.random.fold_in(jax.random.fold_in(streams_of[4], part), 71), part)
    projected_value_heads = scatter_about(part_splits[2], (ROW_LENGTH, KEY_VALUE_HEADS, HEAD_SIZE), 1.0, 6.0, ((0, 16),))
    lengths = jax.random.randint(part_splits[3], (1,), ROW_LENGTH - TOK_DEV + 1, ROW_LENGTH + 1).astype(jnp.int32)
    return dict(queries=queries, key_heads=key_heads, projected_value_heads=projected_value_heads, lengths=lengths)


def reference(queries, key_heads, projected_value_heads, lengths):
    length_now = lengths[0]
    head_count = queries.shape[1]
    kv_heads = key_heads.shape[1]
    head_width = queries.shape[2]
    share = head_count // kv_heads
    block_rows = math.gcd(ROW_LENGTH, 512)
    key_span = min(ROW_LENGTH, WINDOW + block_rows)
    score_scale = head_width ** -0.5
    sink_keys = key_heads[:SINKS].astype(jnp.float32)
    sink_values = projected_value_heads[:SINKS].astype(jnp.float32)
    sink_pos = jnp.arange(SINKS, dtype=jnp.int32)

    def one_block(block_index):
        first_row = (block_index * block_rows).astype(jnp.int32)
        query_pos = first_row + jnp.arange(block_rows, dtype=jnp.int32)
        key_start = jnp.maximum(first_row + block_rows - key_span, 0).astype(jnp.int32)
        near_keys = lax.dynamic_slice_in_dim(key_heads, key_start, key_span, 0).astype(jnp.float32)
        near_values = lax.dynamic_slice_in_dim(projected_value_heads, key_start, key_span, 0).astype(jnp.float32)
        key_pos = key_start + jnp.arange(key_span, dtype=jnp.int32)
        grouped = lax.dynamic_slice_in_dim(queries, first_row, block_rows, 0).astype(jnp.float32)
        grouped = grouped.reshape(block_rows, kv_heads, share, head_width)
        all_keys = jnp.concatenate([near_keys, sink_keys], 0)
        all_values = jnp.concatenate([near_values, sink_values], 0)
        distance = query_pos[:, None] - key_pos[None, :]
        near_ok = ((distance >= 0) & (distance < WINDOW) & (key_pos[None, :] >= SINKS)
                   & (key_pos[None, :] < length_now))
        sink_gap = query_pos[:, None] - sink_pos[None, :]
        sink_ok = (sink_gap >= 0) & (sink_pos[None, :] < length_now)
        visible = jnp.concatenate([near_ok, sink_ok], 1) & (query_pos[:, None] < length_now)
        scores = jnp.einsum("qhgd,khd->hgqk", grouped, all_keys) * score_scale
        masked = jnp.where(visible, scores, -1e30)
        maximum = jnp.max(masked, axis=-1, keepdims=True)
        weights = jnp.where(visible, jnp.exp(scores - maximum), 0.0)
        totals = jnp.sum(weights, axis=-1)
        rounded = lax.optimization_barrier(weights.astype(jnp.bfloat16)).astype(jnp.float32)
        summed = jnp.einsum("hgqk,khd->hgqd", rounded, all_values)
        valid = query_pos < length_now
        result = jnp.where(valid[:, None], summed / jnp.where(valid, totals, 1.0)[..., None], 0.0)
        return result.transpose(2, 0, 1, 3).reshape(block_rows, head_count, head_width).astype(jnp.bfloat16)

    blocks = lax.map(one_block, jnp.arange(ROW_LENGTH // block_rows, dtype=jnp.int32))
    return blocks.reshape(ROW_LENGTH, head_count, head_width)
```

```python
import functools

import jax
import jax.numpy as jnp
from jax import lax
from jax.experimental import pallas as pl
from jax.experimental.pallas import tpu as pltpu
from jax.sharding import PartitionSpec as P

WINDOW = 4096
SINKS = 4
SIDE = 4
BLOCK = 512
HALF = 256
DIM = 256
NM = 4
NP = 8 - NM
C = 1.4426950408889634 / 16.0
NEG = -1e30
KV, Q, O = 0, 1, 2


def kernel(
    len_ref, q_in, kv_in, o_ref,
    kvb, qb, ob, relay, rx, snk, acc, mx, ls,
    ys, yr, xs, xr, ps, pr, ms, mr, ns, nr, ss, sr, loc,
):
    sid = lax.axis_index("seq")
    x = lax.div(sid, SIDE)
    y = lax.rem(sid, SIDE)
    right = lax.rem(y + 1, SIDE)
    left = lax.rem(y + 3, SIDE)
    far = lax.rem(y + 2, SIDE)
    down = lax.rem(x + 1, SIDE)
    up = lax.rem(x + 3, SIDE)

    def dev(xx, yy):
        return {"seq": xx * SIDE + yy}

    def remote(src, dst, s, r, where):
        return pltpu.make_async_remote_copy(
            src_ref=src, dst_ref=dst, send_sem=s, recv_sem=r,
            device_id=where, device_id_type=pl.DeviceIdType.MESH,
        )

    def src(p, n, half):
        if p == KV:
            return kv_in.at[n, half]
        if p == Q:
            return q_in.at[n, half]
        return ob.at[2 * n + half]

    def dst(p, n, half):
        if p == KV:
            return kvb.at[16 + 2 * n + half]
        if p == Q:
            return qb.at[2 * n + half]
        return o_ref.at[n, half]

    def peer(side):
        return right if side == 0 else left

    def direct(p, side, half):
        n = peer(side)
        k = 2 * side + half
        return remote(src(p, n, half), dst(p, y, half), ys.at[p, k], yr.at[p, k], dev(x, n))

    def relay_out(p, side):
        k = 4 + side
        return remote(
            src(p, far, side), relay.at[p, side], ys.at[p, k], yr.at[p, k], dev(x, peer(side))
        )

    def forward(p, side):
        k = 6 + side
        return remote(
            relay.at[p, side], dst(p, peer(1 - side), side), ys.at[p, k], yr.at[p, k],
            dev(x, peer(side)),
        )

    def got_direct(p, side, half):
        k = 2 * side + half
        d = dst(p, peer(1 - side), half)
        remote(d, d, ys.at[p, k], yr.at[p, k], dev(x, peer(1 - side))).wait_recv()

    def got_relay(p, side):
        k = 4 + side
        d = relay.at[p, side]
        remote(d, d, ys.at[p, k], yr.at[p, k], dev(x, peer(1 - side))).wait_recv()

    def got_forward(p, side):
        k = 6 + side
        d = dst(p, far, side)
        remote(d, d, ys.at[p, k], yr.at[p, k], dev(x, peer(1 - side))).wait_recv()

    def x_next(i):
        return remote(kvb.at[16 + i], kvb.at[8 + i], xs.at[i], xr.at[i], dev(down, y))

    def x_plus(i):
        return remote(kvb.at[8 + i], kvb.at[i], ps.at[i], pr.at[i], dev(down, y))

    def x_minus(i):
        return remote(kvb.at[16 + i], rx.at[i - NP], ms.at[i - NP], mr.at[i - NP], dev(up, y))

    def x_wrap(j):
        return remote(rx.at[j], kvb.at[NP + j], ns.at[j], nr.at[j], dev(up, y))

    def x_sink(first):
        return remote(
            kvb.at[16, :, pl.ds(0, 16), :] if first else snk, snk, ss.at[0], sr.at[0], dev(up, y)
        )

    def x_send(i):
        @pl.when(x < 3)
        def _():
            x_next(i).start()

        @pl.when((x < 2) & (i >= NP))
        def _():
            x_minus(i).start()

    relays_plus = (x == 1) | (x == 2)
    relays_wrap = (x == 0) | (x == 3)
    two_back = x >= 2

    lane = lax.broadcasted_iota(jnp.int32, (BLOCK, 128), 1)
    row = lax.rem(lax.broadcasted_iota(jnp.int32, (BLOCK, 128), 0), HALF)

    def update(yq, half, s_parts, v):
        top = s_parts[0]
        for part in s_parts[1:]:
            top = jnp.maximum(top, part)
        old = mx[yq, half]
        new = jnp.maximum(old, jnp.max(top, axis=-1, keepdims=True))
        alpha = jnp.exp2((old - new) * C)
        p_parts = [jnp.exp2((part - new) * C) for part in s_parts]
        total = p_parts[0]
        for part in p_parts[1:]:
            total = total + part
        ls[yq, half] = ls[yq, half] * alpha + total
        mx[yq, half] = new
        weights = jnp.concatenate([part.astype(jnp.bfloat16) for part in p_parts], axis=1)
        scale = jnp.concatenate([alpha, alpha], axis=1)
        acc[yq, half] = acc[yq, half] * scale + jnp.dot(
            weights, v, preferred_element_type=jnp.float32
        )

    def scores(yq, half, k):
        q = qb[2 * yq + half].reshape(BLOCK, DIM)
        return lax.dot_general(
            q, k, (((1,), (1,)), ((), ())), preferred_element_type=jnp.float32
        )

    def task(yq, b, masked):
        k = kvb[pl.ds(2 * b, 2), 0].reshape(BLOCK, DIM)
        v = kvb[pl.ds(2 * b, 2), 1].reshape(BLOCK, DIM)
        for half in range(2):
            s = scores(yq, half, k)
            parts = [s[:, 128 * j : 128 * (j + 1)] for j in range(4)]
            if masked:
                base = (8 + yq - b) * BLOCK + half * HALF
                first = jnp.where((x == 2) & (b == 0), SINKS, 0)
                for j in range(4):
                    key = lane + 128 * j
                    delta = base + row - key
                    ok = (delta >= 0) & (delta < WINDOW) & (key >= first)
                    parts[j] = jnp.where(ok, parts[j], NEG)
            update(yq, half, parts, v)

    def sink_task(yq):
        k = jnp.concatenate([snk[0], jnp.zeros((112, DIM), jnp.bfloat16)], axis=0)
        v = jnp.concatenate([snk[1], jnp.zeros((112, DIM), jnp.bfloat16)], axis=0)
        for half in range(2):
            s = jnp.where(lane < SINKS, scores(yq, half, k), NEG)
            update(yq, half, [s], v)

    def loop(n, body):
        def step(t, carry):
            body(t)
            return carry

        lax.fori_loop(0, n, step, 0)

    def finalize(yq):
        length = len_ref[0]
        for half in range(2):
            inv = 1.0 / jnp.sum(ls[yq, half], axis=-1, keepdims=True)
            first = (x * SIDE + yq) * BLOCK + half * HALF
            ok = first + row < length
            ok = jnp.concatenate([ok, ok], axis=1)
            out = jnp.where(ok, acc[yq, half] * inv, 0.0)
            ob[2 * yq + half] = out.astype(jnp.bfloat16).reshape(2, HALF, DIM)

    def own_out(half):
        return pltpu.make_async_copy(ob.at[2 * y + half], o_ref.at[y, half], loc.at[half])

    def send_out(yq):
        @pl.when(y == yq)
        def _():
            for half in range(2):
                own_out(half).start()

        @pl.when(right == yq)
        def _():
            for half in range(2):
                direct(O, 0, half).start()

        @pl.when(left == yq)
        def _():
            for half in range(2):
                direct(O, 1, half).start()

        @pl.when(far == yq)
        def _():
            for side in range(2):
                relay_out(O, side).start()

    barrier = pltpu.get_barrier_semaphore()
    for where in (dev(x, right), dev(x, left), dev(down, y), dev(up, y)):
        pl.semaphore_signal(barrier, inc=1, device_id=where, device_id_type=pl.DeviceIdType.MESH)
    pl.semaphore_wait(barrier, 4)

    for half in range(2):
        for side in range(2):
            direct(KV, side, half).start()
    mine = [
        pltpu.make_async_copy(kv_in.at[y, half], kvb.at[16 + 2 * y + half], loc.at[2 + half])
        for half in range(2)
    ] + [
        pltpu.make_async_copy(q_in.at[y, half], qb.at[2 * y + half], loc.at[4 + half])
        for half in range(2)
    ]
    for copy in mine:
        copy.start()
    for side in range(2):
        relay_out(KV, side).start()
    for side in range(2):
        direct(Q, side, 0).start()
    for half in range(2):
        mine[half].wait()
        x_send(2 * y + half)

    def init(t):
        for half in range(2):
            mx[t, half] = jnp.full((BLOCK, 128), NEG, jnp.float32)
            ls[t, half] = jnp.zeros((BLOCK, 128), jnp.float32)
            acc[t, half] = jnp.zeros((BLOCK, DIM), jnp.float32)

    loop(SIDE, init)
    for half in range(2):
        for side in range(2):
            got_direct(KV, side, half)
            x_send(2 * peer(1 - side) + half)
    for side in range(2):
        got_relay(KV, side)
        forward(KV, side).start()
    for side in range(2):
        direct(Q, side, 1).start()
    for side in range(2):
        relay_out(Q, side).start()
    mine[2].wait()
    mine[3].wait()
    task(y, 8 + y, True)
    for side in range(2):
        got_forward(KV, side)
        x_send(2 * far + side)

    @pl.when(x == 0)
    def _():
        x_sink(True).start()

    @pl.when(x == 3)
    def _():
        x_sink(False).wait_recv()
        x_sink(False).start()

    @pl.when(relays_wrap)
    def _():
        for j in range(NM):
            x_minus(NP + j).wait_recv()
            x_wrap(j).start()

    loop(y, lambda t: task(y, 8 + t, False))
    for side in range(2):
        for half in range(2):
            got_direct(Q, side, half)

    def neighbour_block(t):
        yq = jnp.where(t == 0, left, right)
        task(yq, 8 + yq, True)
        loop(yq, lambda r: task(yq, 8 + r, False))

    loop(2, neighbour_block)
    for side in range(2):
        got_relay(Q, side)
        forward(Q, side).start()

    near = lambda t: jnp.where(t == 0, y, jnp.where(t == 1, left, right))

    @pl.when(x >= 1)
    def _():
        for n in (y, left, right):
            for half in range(2):
                x_next(2 * n + half).wait_recv()
        loop(9, lambda t: task(near(lax.div(t, 3)), 4 + near(lax.rem(t, 3)), False))
        for half in range(2):
            x_next(2 * far + half).wait_recv()

    @pl.when(relays_plus)
    def _():
        for i in reversed(range(NP)):
            x_plus(i).start()

    for side in range(2):
        got_forward(Q, side)
    task(far, 8 + far, True)
    loop(far, lambda r: task(far, 8 + r, False))

    @pl.when(x >= 1)
    def _():
        def rest(t):
            yq = jnp.where(t < 4, far, near(t - 4))
            n = jnp.where(t < 3, near(t), far)
            task(yq, 4 + n, False)

        loop(7, rest)

    @pl.when(two_back)
    def _():
        @pl.when(x == 2)
        def _():
            x_sink(False).wait_recv()

        loop(SIDE, sink_task)
        for j in range(NM):
            x_wrap(j).wait_recv()
        loop(2, lambda t: task(3 - t, 3 - t, True))
        loop(
            5,
            lambda t: task(
                jnp.where(t < 3, 2 - t, 4 - t), jnp.where(t < 3, 3, 2), False
            ),
        )

    for yq in (3, 2):
        finalize(yq)
        send_out(yq)

    def forward_out(late):
        for side in range(2):
            n = peer(side)

            @pl.when((n < 2) if late else (n >= 2))
            def _():
                got_relay(O, side)
                forward(O, side).start()

    @pl.when(two_back)
    def _():
        x_plus(3).wait_recv()
        x_plus(2).wait_recv()
        task(jnp.int32(0), jnp.int32(1), False)
        task(jnp.int32(1), jnp.int32(1), True)

    finalize(1)
    send_out(1)
    forward_out(False)

    @pl.when(two_back)
    def _():
        x_plus(1).wait_recv()
        x_plus(0).wait_recv()
        task(jnp.int32(0), jnp.int32(0), True)

    finalize(0)
    send_out(0)
    forward_out(True)

    for side in range(2):
        for half in range(2):
            got_direct(O, side, half)
        got_forward(O, side)
    for half in range(2):
        own_out(half).wait()
    for p in (KV, Q, O):
        for side in range(2):
            for half in range(2):
                direct(p, side, half).wait_send()
            relay_out(p, side).wait_send()
            forward(p, side).wait_send()

    @pl.when(x < 3)
    def _():
        for i in range(8):
            x_next(i).wait_send()

    @pl.when(relays_plus)
    def _():
        for i in range(NP):
            x_plus(i).wait_send()

    @pl.when(x < 2)
    def _():
        for i in range(NP, 8):
            x_minus(i).wait_send()

    @pl.when(relays_wrap)
    def _():
        for j in range(NM):
            x_wrap(j).wait_send()
        x_sink(False).wait_send()


def attend(lengths, q, kv):
    bf = jnp.bfloat16
    dma = pltpu.SemaphoreType.DMA
    any_space = pl.BlockSpec(memory_space=pl.ANY)
    return pl.pallas_call(
        kernel,
        name="window_attention",
        out_shape=jax.ShapeDtypeStruct(q.shape, bf),
        in_specs=[pl.BlockSpec(memory_space=pltpu.SMEM), any_space, any_space],
        out_specs=any_space,
        scratch_shapes=[
            pltpu.VMEM((24, 2, HALF, DIM), bf),
            pltpu.VMEM((8, 2, HALF, DIM), bf),
            pltpu.VMEM((8, 2, HALF, DIM), bf),
            pltpu.VMEM((3, 2, 2, HALF, DIM), bf),
            pltpu.VMEM((NM, 2, HALF, DIM), bf),
            pltpu.VMEM((2, 16, DIM), bf),
            pltpu.VMEM((SIDE, 2, BLOCK, DIM), jnp.float32),
            pltpu.VMEM((SIDE, 2, BLOCK, 128), jnp.float32),
            pltpu.VMEM((SIDE, 2, BLOCK, 128), jnp.float32),
            dma((3, 8)), dma((3, 8)),
            dma((8,)), dma((8,)),
            dma((NP,)), dma((NP,)),
            dma((NM,)), dma((NM,)),
            dma((NM,)), dma((NM,)),
            dma((1,)), dma((1,)),
            dma((6,)),
        ],
        compiler_params=pltpu.CompilerParams(
            collective_id=0, has_side_effects=True, vmem_limit_bytes=56 * 1024 * 1024
        ),
    )(lengths, q, kv)


def shards(queries, key_heads, projected_value_heads, lengths):
    tok = queries.shape[0]
    q = queries.reshape(2, HALF, SIDE, 2, DIM).transpose(2, 0, 3, 1, 4)
    kv = jnp.stack([key_heads, projected_value_heads]).reshape(2, 2, HALF, SIDE, DIM)
    kv = kv.transpose(3, 1, 0, 2, 4)
    out = attend(lengths, q, kv)
    return out.transpose(1, 3, 0, 2, 4).reshape(tok, 2 * SIDE, DIM)


def solution(mesh):
    in_specs = (
        P(("batch", "seq"), None, None),
        P(("batch", "seq"), None, None),
        P(("batch", "seq"), None, None),
        P("batch"),
    )
    out_specs = P(("batch", "seq"), None, None)
    return jax.shard_map(shards, mesh=mesh, in_specs=in_specs, out_specs=out_specs, check_vma=False)
```

```python
import functools

import jax
import jax.numpy as jnp
from jax import lax
from jax.experimental import pallas as pl
from jax.experimental.pallas import tpu as pltpu
from jax.sharding import PartitionSpec as P

SINKS = 4
SIDE = 4
BLOCK = 512
HALF = 256
DIM = 256
NM = 5
NP = 8 - NM
C = 1.4426950408889634 / 16.0
NEG = -1e30
K, V, Q, O = 0, 1, 2, 3
FULL, DIAG, EDGE = 0, 1, 2


def kernel(
    len_ref, q_in, k_in, v_in, o_ref,
    kvb, qb, ob, rx, snk, acc0, acc1, mx0, mx1, ls0, ls1, sc0, sc1,
    ys, yr, xs, xr, ps, pr, ms, mr, ns, nr, ss, sr, loc,
):
    accs, mxs, lss, scs = (acc0, acc1), (mx0, mx1), (ls0, ls1), (sc0, sc1)
    sid = lax.axis_index("seq")
    x = lax.div(sid, SIDE)
    y = lax.rem(sid, SIDE)
    right = lax.rem(y + 1, SIDE)
    left = lax.rem(y + 3, SIDE)
    far = lax.rem(y + 2, SIDE)
    down = lax.rem(x + 1, SIDE)
    up = lax.rem(x + 3, SIDE)

    def dev(xx, yy):
        return {"seq": xx * SIDE + yy}

    def remote(src, dst, s, r, where):
        return pltpu.make_async_remote_copy(
            src_ref=src, dst_ref=dst, send_sem=s, recv_sem=r,
            device_id=where, device_id_type=pl.DeviceIdType.MESH,
        )

    def rows(half):
        return pl.ds(half * HALF, HALF)

    def src(p, n, half):
        if p == K:
            return k_in.at[n, rows(half)]
        if p == V:
            return v_in.at[n, rows(half)]
        if p == Q:
            return q_in.at[pl.ds(2 * n, 2), rows(half)]
        return ob.at[2 * n + half]

    def dst(p, n, half):
        if p in (K, V):
            return kvb.at[16 + 2 * n + half, p]
        if p == Q:
            return qb.at[2 * n + half]
        return o_ref.at[pl.ds(2 * n, 2), rows(half)]

    to = (right, left, far)
    come = (left, right, far)

    def send(p, side, half):
        k = 2 * side + half
        return remote(
            src(p, to[side], half), dst(p, y, half), ys.at[p, k], yr.at[p, k], dev(x, to[side])
        )

    def got(p, side, half):
        k = 2 * side + half
        d = dst(p, come[side], half)
        remote(d, d, ys.at[p, k], yr.at[p, k], dev(x, come[side])).wait_recv()

    def x_next(i):
        return remote(kvb.at[16 + i], kvb.at[8 + i], xs.at[i], xr.at[i], dev(down, y))

    def x_plus(i):
        return remote(kvb.at[8 + i], kvb.at[i], ps.at[i], pr.at[i], dev(down, y))

    def x_minus(i):
        return remote(kvb.at[16 + i], rx.at[i - NP], ms.at[i - NP], mr.at[i - NP], dev(up, y))

    def x_wrap(j):
        return remote(rx.at[j], kvb.at[NP + j], ns.at[j], nr.at[j], dev(up, y))

    def x_sink(first):
        return remote(
            kvb.at[16, :, pl.ds(0, 16), :] if first else snk, snk, ss.at[0], sr.at[0], dev(up, y)
        )

    def x_send(i):
        @pl.when(x < 3)
        def _():
            x_next(i).start()

        @pl.when((x < 2) & (i >= NP))
        def _():
            x_minus(i).start()

    relays_plus = (x == 1) | (x == 2)
    relays_wrap = (x == 0) | (x == 3)
    two_back = x >= 2

    lane = lax.broadcasted_iota(jnp.int32, (BLOCK, 128), 1)
    row = lax.rem(lax.broadcasted_iota(jnp.int32, (BLOCK, 128), 0), HALF)

    def scores(yq, half, k):
        q = qb[2 * yq + half].reshape(BLOCK, DIM)
        return lax.dot_general(
            q, k, (((1,), (1,)), ((), ())), preferred_element_type=jnp.float32
        )

    def update(yq, half, parts, v):
        acc, mx, ls = accs[half], mxs[half], lss[half]
        top = parts[0]
        for part in parts[1:]:
            top = jnp.maximum(top, part)
        old = mx[yq]
        new = jnp.maximum(old, jnp.max(top, axis=-1, keepdims=True))
        alpha = jnp.exp2((old - new) * C)
        weights = [jnp.exp2((part - new) * C) for part in parts]
        total = weights[0]
        for part in weights[1:]:
            total = total + part
        ls[yq] = ls[yq] * alpha + total
        mx[yq] = new
        rounded = jnp.concatenate([part.astype(jnp.bfloat16) for part in weights], axis=1)
        scale = jnp.concatenate([alpha, alpha], axis=1)
        acc[yq] = acc[yq] * scale + jnp.dot(rounded, v, preferred_element_type=jnp.float32)

    def cols(s):
        return [s[:, 128 * j : 128 * (j + 1)] for j in range(s.shape[1] // 128)]

    def keys_of(piece, n):
        return kvb[pl.ds(piece, n), 0].reshape(n * HALF, DIM)

    def values_of(piece, n):
        return kvb[pl.ds(piece, n), 1].reshape(n * HALF, DIM)

    def tiles(yq, half, piece, modes):
        n = len(modes)
        parts = cols(scores(yq, half, keys_of(piece, n)))
        for j in range(2 * n):
            key = lane + 128 * (j % 2)
            if modes[j // 2] == DIAG:
                parts[j] = jnp.where(key <= row, parts[j], NEG)
            if modes[j // 2] == EDGE:
                ok = key > row
                if half == 0 and j == 0:
                    ok = ok & (key >= jnp.where((x == 2) & (yq == 0), SINKS, 0))
                parts[j] = jnp.where(ok, parts[j], NEG)
        update(yq, half, parts, values_of(piece, n))

    def diag(yq):
        tiles(yq, 0, 16 + 2 * yq, [DIAG])
        tiles(yq, 1, 16 + 2 * yq, [FULL, DIAG])

    def edge(yq):
        tiles(yq, 0, 2 * yq, [EDGE, FULL])
        tiles(yq, 1, 2 * yq + 1, [EDGE])

    def loop(n, body):
        def step(t, carry):
            body(t)
            return carry

        lax.fori_loop(0, n, step, 0)

    def pipe(n, get):
        def qk(t, half):
            yq, b = get(t)
            scs[half][...] = scores(yq, half, keys_of(2 * b, 2))

        def softmax(t, half):
            yq, b = get(t)
            update(yq, half, cols(scs[half][...]), values_of(2 * b, 2))

        def step(t):
            qk(t, 1)
            softmax(t, 0)
            qk(jnp.minimum(t + 1, n - 1), 0)
            softmax(t, 1)

        @pl.when(n > 0)
        def _():
            qk(0, 0)
            loop(n, step)

    def sink_task(yq):
        pad = jnp.zeros((112, DIM), jnp.bfloat16)
        k = jnp.concatenate([snk[0], pad], axis=0)
        v = jnp.concatenate([snk[1], pad], axis=0)
        for half in range(2):
            update(yq, half, [jnp.where(lane < SINKS, scores(yq, half, k), NEG)], v)

    def finalize(yq, half):
        inv = 1.0 / jnp.sum(lss[half][yq], axis=-1, keepdims=True)
        ok = (x * SIDE + yq) * BLOCK + half * HALF + row < len_ref[0]
        ok = jnp.concatenate([ok, ok], axis=1)
        out = jnp.where(ok, accs[half][yq] * inv, 0.0)
        ob[2 * yq + half] = out.astype(jnp.bfloat16).reshape(2, HALF, DIM)

    def own_out(half):
        return pltpu.make_async_copy(ob.at[2 * y + half], dst(O, y, half), loc.at[half])

    def send_out(yq, half):
        @pl.when(y == yq)
        def _():
            own_out(half).start()

        for side in range(3):

            @pl.when(to[side] == yq)
            def _():
                send(O, side, half).start()

    barrier = pltpu.get_barrier_semaphore()
    for where in (dev(x, right), dev(x, left), dev(x, far), dev(down, y), dev(up, y)):
        pl.semaphore_signal(barrier, inc=1, device_id=where, device_id_type=pl.DeviceIdType.MESH)
    pl.semaphore_wait(barrier, 5)

    mine = [
        pltpu.make_async_copy(src(p, y, half), dst(p, y, half), loc.at[2 + 2 * p + half])
        for p in (K, V, Q)
        for half in range(2)
    ]
    for half in range(2):
        for side in range(2):
            send(K, side, half).start()
            send(V, side, half).start()
    for copy in mine:
        copy.start()
    for half in range(2):
        for side in range(2):
            send(Q, side, half).start()
    for half in range(2):
        send(K, 2, half).start()
        send(V, 2, half).start()
    for half in range(2):
        send(Q, 2, half).start()
    for half in range(2):
        mine[half].wait()
        mine[2 + half].wait()
        x_send(2 * y + half)

    def init(t):
        for half in range(2):
            mxs[half][t] = jnp.full((BLOCK, 128), NEG, jnp.float32)
            lss[half][t] = jnp.zeros((BLOCK, 128), jnp.float32)
            accs[half][t] = jnp.zeros((BLOCK, DIM), jnp.float32)

    loop(SIDE, init)
    mine[4].wait()
    mine[5].wait()
    diag(y)
    for side in range(2):
        for half in range(2):
            got(K, side, half)
            got(V, side, half)
            x_send(2 * come[side] + half)

    def sink_start():
        x_sink(True).start()

    pl.when((x == 0) & (far != 0))(sink_start)

    lower = (left < y).astype(jnp.int32) + (right < y).astype(jnp.int32)

    @pl.when(x >= 1)
    def _():
        for half in range(2):
            x_next(2 * y + half).wait_recv()

    def own_tasks(t):
        return y, jnp.where(t < lower, 8 + jnp.where(t == 0, left, right), 4 + y)

    pipe(lower + (x >= 1).astype(jnp.int32), own_tasks)
    for half in range(2):
        for side in range(2):
            got(Q, side, half)

    def near(i):
        return i + (i >= far).astype(jnp.int32)

    loop(2, lambda t: diag(jnp.where(t == 0, left, right)))

    @pl.when(x >= 1)
    def _():
        for half in range(2):
            x_next(2 * left + half).wait_recv()

    pairs = 3 - lower
    start = ((y == 1) | (y == 2)).astype(jnp.int32)

    def near_tasks(t):
        own = t < pairs
        i = jnp.minimum(t + start, 2)
        r = t - pairs
        yq = jnp.where(
            own, near(jnp.minimum(i + 1, 2)), jnp.where(r == 0, left, jnp.where(r == 1, right, near(r - 2)))
        )
        b = jnp.where(own, 8 + near(i >> 1), 4 + jnp.where(r < 2, y, left))
        return yq, b

    pipe(pairs + jnp.where(x >= 1, 5, 0), near_tasks)

    def wrap_relays(late):
        @pl.when(relays_wrap)
        def _():
            for j in range(NM):
                i = NP + j

                @pl.when((far == i // 2) if late else (far != i // 2))
                def _():
                    x_minus(i).wait_recv()
                    x_wrap(j).start()

    wrap_relays(False)
    for half in range(2):
        got(K, 2, half)
        got(V, 2, half)
        x_send(2 * far + half)

    pl.when((x == 0) & (far == 0))(sink_start)

    @pl.when(x == 3)
    def _():
        x_sink(False).wait_recv()
        x_sink(False).start()

    @pl.when(x >= 1)
    def _():
        for half in range(2):
            x_next(2 * right + half).wait_recv()

    def right_tasks(t):
        t = t + jnp.where(x >= 1, 0, 3)
        yq = jnp.where(t < 3, near(t), near(far + t - 3))
        return yq, jnp.where(t < 3, 4 + right, 8 + far)

    pipe(jnp.where(x >= 1, 6, 3) - far, right_tasks)

    @pl.when(relays_plus)
    def _():
        @pl.when(far != 1)
        def _():
            x_plus(2).start()

        @pl.when(far >= 2)
        def _():
            x_plus(1).start()
            x_plus(0).start()

    wrap_relays(True)

    def early(b):
        return (x == 2) & (far != b)

    def wait_back(b):
        for half in range(2):
            x_wrap(2 * b + half - NP).wait_recv()

    @pl.when(two_back)
    def _():
        @pl.when(x == 2)
        def _():
            x_sink(False).wait_recv()

        loop(3, lambda t: sink_task(near(t)))

    def early_block(i):
        b = 3 - i

        @pl.when(early(b))
        def _():
            wait_back(b)
            edge(b)
            pipe(b - (far < b).astype(jnp.int32), lambda t: (near(t), b))

    loop(2, early_block)

    @pl.when(x >= 1)
    def _():
        for half in range(2):
            x_next(2 * far + half).wait_recv()

    @pl.when(relays_plus)
    def _():
        @pl.when(far == 1)
        def _():
            x_plus(2).start()

        @pl.when(far < 2)
        def _():
            x_plus(1).start()
            x_plus(0).start()

    for half in range(2):
        got(Q, 2, half)
    diag(far)

    def far_tasks(t):
        t = t + jnp.where(x >= 1, 0, 7)
        return jnp.where(t < 3, near(t), far), jnp.where(t < 3, 4 + far, t + 1)

    pipe(jnp.where(x >= 1, 7, 0) + far, far_tasks)

    pl.when(two_back)(lambda: sink_task(far))

    def late_block(i):
        b = 3 - i
        late = two_back & jnp.logical_not(early(b))

        @pl.when(late)
        def _():
            wait_back(b)
            edge(b)

        for half in range(2):
            finalize(b, half)
        for half in range(2):
            send_out(b, half)
        n = jnp.where(late, b, jnp.where(two_back & (far < b), 1, 0))
        pipe(n, lambda t: (jnp.where(late, t, far), b))

    loop(2, late_block)

    @pl.when(two_back)
    def _():
        x_wrap(3 - NP).wait_recv()
        tiles(1, 1, 3, [EDGE])

    finalize(1, 1)
    send_out(1, 1)

    @pl.when(two_back)
    def _():
        x_plus(2).wait_recv()
        tiles(1, 0, 2, [EDGE, FULL])

    finalize(1, 0)
    send_out(1, 0)

    @pl.when(two_back)
    def _():
        for half in range(2):
            tiles(0, half, 2, [FULL, FULL])
        x_plus(1).wait_recv()
        tiles(0, 1, 1, [EDGE])

    finalize(0, 1)
    send_out(0, 1)

    @pl.when(two_back)
    def _():
        tiles(0, 0, 1, [FULL])
        x_plus(0).wait_recv()
        tiles(0, 0, 0, [EDGE])

    finalize(0, 0)
    send_out(0, 0)

    for half in range(2):
        for side in range(3):
            got(O, side, half)
        own_out(half).wait()
    for p in (K, V, Q, O):
        for side in range(3):
            for half in range(2):
                send(p, side, half).wait_send()

    @pl.when(x < 3)
    def _():
        for i in range(8):
            x_next(i).wait_send()

    @pl.when(relays_plus)
    def _():
        for i in range(NP):
            x_plus(i).wait_send()

    @pl.when(x < 2)
    def _():
        for i in range(NP, 8):
            x_minus(i).wait_send()

    @pl.when(relays_wrap)
    def _():
        for j in range(NM):
            x_wrap(j).wait_send()
        x_sink(False).wait_send()


def attend(lengths, q, k, v):
    bf = jnp.bfloat16
    dma = pltpu.SemaphoreType.DMA
    any_space = pl.BlockSpec(memory_space=pl.ANY)
    return pl.pallas_call(
        kernel,
        name="window_attention",
        out_shape=jax.ShapeDtypeStruct(q.shape, bf),
        in_specs=[pl.BlockSpec(memory_space=pltpu.SMEM), any_space, any_space, any_space],
        out_specs=any_space,
        scratch_shapes=[
            pltpu.VMEM((24, 2, HALF, DIM), bf),
            pltpu.VMEM((8, 2, HALF, DIM), bf),
            pltpu.VMEM((8, 2, HALF, DIM), bf),
            pltpu.VMEM((NM, 2, HALF, DIM), bf),
            pltpu.VMEM((2, 16, DIM), bf),
            *[pltpu.VMEM((SIDE, BLOCK, DIM), jnp.float32)] * 2,
            *[pltpu.VMEM((SIDE, BLOCK, 128), jnp.float32)] * 4,
            *[pltpu.VMEM((BLOCK, BLOCK), jnp.float32)] * 2,
            dma((4, 6)), dma((4, 6)),
            dma((8,)), dma((8,)),
            dma((NP,)), dma((NP,)),
            dma((NM,)), dma((NM,)),
            dma((NM,)), dma((NM,)),
            dma((1,)), dma((1,)),
            dma((8,)),
        ],
        compiler_params=pltpu.CompilerParams(
            collective_id=0, has_side_effects=True, vmem_limit_bytes=56 * 1024 * 1024
        ),
    )(lengths, q, k, v)


def shards(queries, key_heads, projected_value_heads, lengths):
    q, k, v = (z.transpose(1, 0, 2) for z in (queries, key_heads, projected_value_heads))
    return attend(lengths, q, k, v).transpose(1, 0, 2)


def solution(mesh):
    in_specs = (
        P(("batch", "seq"), None, None),
        P(("batch", "seq"), None, None),
        P(("batch", "seq"), None, None),
        P("batch"),
    )
    out_specs = P(("batch", "seq"), None, None)
    return jax.shard_map(shards, mesh=mesh, in_specs=in_specs, out_specs=out_specs, check_vma=False)
```

```python
import functools

import jax
import jax.numpy as jnp
from jax import lax
from jax.experimental import pallas as pl
from jax.experimental.pallas import tpu as pltpu
from jax.sharding import PartitionSpec as P

SINKS = 4
SIDE = 4
BLOCK = 512
HALF = 256
DIM = 256
NM = 5
NP = 8 - NM
C = 1.4426950408889634 / 16.0
NEG = -1e30
K, V, Q, O = 0, 1, 2, 3
FULL, DIAG, EDGE = 0, 1, 2


def kernel(
    len_ref, q_in, k_in, v_in, o_ref,
    kvb, qb, ob, rx, snk, acc0, acc1, mx0, mx1, ls0, ls1, sc0, sc1,
    ys, yr, xs, xr, ps, pr, ms, mr, ns, nr, ss, sr, ks, kr, loc,
):
    accs, mxs, lss, scs = (acc0, acc1), (mx0, mx1), (ls0, ls1), (sc0, sc1)
    sid = lax.axis_index("seq")
    x = lax.div(sid, SIDE)
    y = lax.rem(sid, SIDE)
    right = lax.rem(y + 1, SIDE)
    left = lax.rem(y + 3, SIDE)
    far = lax.rem(y + 2, SIDE)
    down = lax.rem(x + 1, SIDE)
    up = lax.rem(x + 3, SIDE)

    def dev(xx, yy):
        return {"seq": xx * SIDE + yy}

    def remote(src, dst, s, r, where):
        return pltpu.make_async_remote_copy(
            src_ref=src, dst_ref=dst, send_sem=s, recv_sem=r,
            device_id=where, device_id_type=pl.DeviceIdType.MESH,
        )

    def rows(half):
        return pl.ds(half * HALF, HALF)

    def src(p, n, half):
        if p == K:
            return k_in.at[n, rows(half)]
        if p == V:
            return v_in.at[n, rows(half)]
        if p == Q:
            return q_in.at[pl.ds(2 * n, 2), rows(half)]
        return ob.at[2 * n + half]

    def dst(p, n, half):
        if p in (K, V):
            return kvb.at[16 + 2 * n + half, p]
        if p == Q:
            return qb.at[2 * n + half]
        return o_ref.at[pl.ds(2 * n, 2), rows(half)]

    to = (right, left, far)
    come = (left, right, far)

    def send(p, side, half):
        k = 2 * side + half
        return remote(
            src(p, to[side], half), dst(p, y, half), ys.at[p, k], yr.at[p, k], dev(x, to[side])
        )

    def got(p, side, half):
        k = 2 * side + half
        d = dst(p, come[side], half)
        remote(d, d, ys.at[p, k], yr.at[p, k], dev(x, come[side])).wait_recv()

    def x_next(i):
        return remote(kvb.at[16 + i], kvb.at[8 + i], xs.at[i], xr.at[i], dev(down, y))

    def x_plus(i):
        return remote(kvb.at[8 + i], kvb.at[i], ps.at[i], pr.at[i], dev(down, y))

    def x_minus(i):
        return remote(kvb.at[16 + i], rx.at[i - NP], ms.at[i - NP], mr.at[i - NP], dev(up, y))

    def x_wrap(j):
        return remote(rx.at[j], kvb.at[NP + j], ns.at[j], nr.at[j], dev(up, y))

    def x_sink():
        return remote(snk, snk, ss.at[0], sr.at[0], dev(up, y))

    def sink_rows(p, n):
        return (k_in if p == K else v_in).at[n, pl.ds(0, 16)]

    def sink_out(p, side):
        n = to[side]
        return remote(sink_rows(p, n), snk.at[p], ks.at[p, side], kr.at[p], dev(x, n))

    def sink_own(p):
        return pltpu.make_async_copy(sink_rows(p, y), snk.at[p], loc.at[8 + p])

    def x_send(i):
        @pl.when(x < 3)
        def _():
            x_next(i).start()

        @pl.when((x < 2) & (i >= NP))
        def _():
            x_minus(i).start()

    relays_plus = (x == 1) | (x == 2)
    relays_wrap = (x == 0) | (x == 3)
    two_back = x >= 2

    lane = lax.broadcasted_iota(jnp.int32, (BLOCK, 128), 1)
    row = lax.rem(lax.broadcasted_iota(jnp.int32, (BLOCK, 128), 0), HALF)

    def scores(yq, half, k):
        q = qb[2 * yq + half].reshape(BLOCK, DIM)
        return lax.dot_general(
            q, k, (((1,), (1,)), ((), ())), preferred_element_type=jnp.float32
        )

    def update(yq, half, parts, v):
        acc, mx, ls = accs[half], mxs[half], lss[half]
        top = parts[0]
        for part in parts[1:]:
            top = jnp.maximum(top, part)
        old = mx[yq]
        new = jnp.maximum(old, jnp.max(top, axis=-1, keepdims=True))
        alpha = jnp.exp2((old - new) * C)
        weights = [jnp.exp2((part - new) * C) for part in parts]
        total = weights[0]
        for part in weights[1:]:
            total = total + part
        ls[yq] = ls[yq] * alpha + total
        mx[yq] = new
        rounded = jnp.concatenate([part.astype(jnp.bfloat16) for part in weights], axis=1)
        scale = jnp.concatenate([alpha, alpha], axis=1)
        acc[yq] = acc[yq] * scale + jnp.dot(rounded, v, preferred_element_type=jnp.float32)

    def cols(s):
        return [s[:, 128 * j : 128 * (j + 1)] for j in range(s.shape[1] // 128)]

    def keys_of(piece, n):
        return kvb[pl.ds(piece, n), 0].reshape(n * HALF, DIM)

    def values_of(piece, n):
        return kvb[pl.ds(piece, n), 1].reshape(n * HALF, DIM)

    def tiles(yq, half, piece, modes):
        n = len(modes)
        parts = cols(scores(yq, half, keys_of(piece, n)))
        for j in range(2 * n):
            key = lane + 128 * (j % 2)
            if modes[j // 2] == DIAG:
                parts[j] = jnp.where(key <= row, parts[j], NEG)
            if modes[j // 2] == EDGE:
                ok = key > row
                if half == 0 and j == 0:
                    ok = ok & (key >= jnp.where((x == 2) & (yq == 0), SINKS, 0))
                parts[j] = jnp.where(ok, parts[j], NEG)
        update(yq, half, parts, values_of(piece, n))

    def diag(yq):
        tiles(yq, 0, 16 + 2 * yq, [DIAG])
        tiles(yq, 1, 16 + 2 * yq, [FULL, DIAG])

    def edge(yq):
        tiles(yq, 0, 2 * yq, [EDGE, FULL])
        tiles(yq, 1, 2 * yq + 1, [EDGE])

    def loop(n, body):
        def step(t, carry):
            body(t)
            return carry

        lax.fori_loop(0, n, step, 0)

    def pipe(n, get):
        def qk(t, half):
            yq, b = get(t)
            scs[half][...] = scores(yq, half, keys_of(2 * b, 2))

        def softmax(t, half):
            yq, b = get(t)
            update(yq, half, cols(scs[half][...]), values_of(2 * b, 2))

        def step(t):
            qk(t, 1)
            softmax(t, 0)
            qk(jnp.minimum(t + 1, n - 1), 0)
            softmax(t, 1)

        @pl.when(n > 0)
        def _():
            qk(0, 0)
            loop(n, step)

    def sink_task(yq):
        pad = jnp.zeros((112, DIM), jnp.bfloat16)
        k = jnp.concatenate([snk[0], pad], axis=0)
        v = jnp.concatenate([snk[1], pad], axis=0)
        for half in range(2):
            update(yq, half, [jnp.where(lane < SINKS, scores(yq, half, k), NEG)], v)

    def finalize(yq, half):
        inv = 1.0 / jnp.sum(lss[half][yq], axis=-1, keepdims=True)
        ok = (x * SIDE + yq) * BLOCK + half * HALF + row < len_ref[0]
        ok = jnp.concatenate([ok, ok], axis=1)
        out = jnp.where(ok, accs[half][yq] * inv, 0.0)
        ob[2 * yq + half] = out.astype(jnp.bfloat16).reshape(2, HALF, DIM)

    def own_out(half):
        return pltpu.make_async_copy(ob.at[2 * y + half], dst(O, y, half), loc.at[half])

    def send_out(yq, half):
        @pl.when(y == yq)
        def _():
            own_out(half).start()

        for side in range(3):

            @pl.when(to[side] == yq)
            def _():
                send(O, side, half).start()

    barrier = pltpu.get_barrier_semaphore()
    for where in (dev(x, right), dev(x, left), dev(x, far), dev(down, y), dev(up, y)):
        pl.semaphore_signal(barrier, inc=1, device_id=where, device_id_type=pl.DeviceIdType.MESH)
    pl.semaphore_wait(barrier, 5)

    mine = [
        pltpu.make_async_copy(src(p, y, half), dst(p, y, half), loc.at[2 + 2 * p + half])
        for p in (K, V, Q)
        for half in range(2)
    ]

    @pl.when(sid == 0)
    def _():
        for p in (K, V):
            for side in range(3):
                sink_out(p, side).start()
            sink_own(p).start()

    for half in range(2):
        for side in range(2):
            send(K, side, half).start()
            send(V, side, half).start()
    for copy in mine:
        copy.start()
    for half in range(2):
        for side in range(2):
            send(Q, side, half).start()
    for half in range(2):
        send(K, 2, half).start()
        send(V, 2, half).start()
    for half in range(2):
        send(Q, 2, half).start()
    for half in range(2):
        mine[half].wait()
        mine[2 + half].wait()
        x_send(2 * y + half)

    @pl.when(sid == 0)
    def _():
        for p in (K, V):
            sink_own(p).wait()

    @pl.when((x == 0) & (y > 0))
    def _():
        for p in (K, V):
            remote(snk.at[p], snk.at[p], ks.at[p, 0], kr.at[p], dev(x, y)).wait_recv()

    @pl.when(x == 0)
    def _():
        x_sink().start()

    def init(t):
        for half in range(2):
            mxs[half][t] = jnp.full((BLOCK, 128), NEG, jnp.float32)
            lss[half][t] = jnp.zeros((BLOCK, 128), jnp.float32)
            accs[half][t] = jnp.zeros((BLOCK, DIM), jnp.float32)

    loop(SIDE, init)
    mine[4].wait()
    mine[5].wait()
    diag(y)
    for side in range(2):
        for half in range(2):
            got(K, side, half)
            got(V, side, half)
            x_send(2 * come[side] + half)

    def wrap(n):
        for half in range(2):
            i = 2 * n + half

            @pl.when(relays_wrap & (i >= NP))
            def _():
                x_minus(i).wait_recv()
                x_wrap(i - NP).start()

    lower = (left < y).astype(jnp.int32) + (right < y).astype(jnp.int32)

    @pl.when(x >= 1)
    def _():
        for half in range(2):
            x_next(2 * y + half).wait_recv()

    def own_tasks(t):
        return y, jnp.where(t < lower, 8 + jnp.where(t == 0, left, right), 4 + y)

    pipe(lower + (x >= 1).astype(jnp.int32), own_tasks)
    wrap(y)

    @pl.when(x == 3)
    def _():
        x_sink().wait_recv()
        x_sink().start()

    for half in range(2):
        for side in range(2):
            got(Q, side, half)

    def near(i):
        return i + (i >= far).astype(jnp.int32)

    loop(2, lambda t: diag(jnp.where(t == 0, left, right)))
    wrap(left)

    @pl.when(x >= 1)
    def _():
        for half in range(2):
            x_next(2 * left + half).wait_recv()

    pairs = 3 - lower
    start = ((y == 1) | (y == 2)).astype(jnp.int32)

    def near_tasks(t):
        own = t < pairs
        i = jnp.minimum(t + start, 2)
        r = t - pairs
        yq = jnp.where(
            own, near(jnp.minimum(i + 1, 2)), jnp.where(r == 0, left, jnp.where(r == 1, right, near(r - 2)))
        )
        b = jnp.where(own, 8 + near(i >> 1), 4 + jnp.where(r < 2, y, left))
        return yq, b

    pipe(pairs + jnp.where(x >= 1, 5, 0), near_tasks)

    wrap(right)
    for half in range(2):
        got(K, 2, half)
        got(V, 2, half)
        x_send(2 * far + half)

    @pl.when(x >= 1)
    def _():
        for half in range(2):
            x_next(2 * right + half).wait_recv()

    def right_tasks(t):
        t = t + jnp.where(x >= 1, 0, 3)
        yq = jnp.where(t < 3, near(t), near(far + t - 3))
        return yq, jnp.where(t < 3, 4 + right, 8 + far)

    pipe(jnp.where(x >= 1, 6, 3) - far, right_tasks)

    @pl.when(relays_plus)
    def _():
        @pl.when(far != 1)
        def _():
            x_plus(2).start()

        @pl.when(far >= 2)
        def _():
            x_plus(1).start()
            x_plus(0).start()


    def early(b):
        return (x == 2) & ((b == y) | (b == left))

    def wait_back(b):
        for half in range(2):
            x_wrap(2 * b + half - NP).wait_recv()

    @pl.when(two_back)
    def _():
        @pl.when(x == 2)
        def _():
            x_sink().wait_recv()

        loop(3, lambda t: sink_task(near(t)))

    def early_block(i):
        b = 3 - i

        @pl.when(early(b))
        def _():
            wait_back(b)
            edge(b)
            pipe(b - (far < b).astype(jnp.int32), lambda t: (near(t), b))

    loop(2, early_block)

    @pl.when(x >= 1)
    def _():
        for half in range(2):
            x_next(2 * far + half).wait_recv()

    @pl.when(relays_plus)
    def _():
        @pl.when(far == 1)
        def _():
            x_plus(2).start()

        @pl.when(far < 2)
        def _():
            x_plus(1).start()
            x_plus(0).start()

    wrap(far)
    for half in range(2):
        got(Q, 2, half)
    diag(far)

    def far_tasks(t):
        t = t + jnp.where(x >= 1, 0, 7)
        return jnp.where(t < 3, near(t), far), jnp.where(t < 3, 4 + far, t + 1)

    pipe(jnp.where(x >= 1, 7, 0) + far, far_tasks)

    pl.when(two_back)(lambda: sink_task(far))

    def late_block(i):
        b = 3 - i
        late = two_back & jnp.logical_not(early(b))

        @pl.when(late)
        def _():
            wait_back(b)
            edge(b)

        for half in range(2):
            finalize(b, half)
        for half in range(2):
            send_out(b, half)
        n = jnp.where(late, b, jnp.where(two_back & (far < b), 1, 0))
        pipe(n, lambda t: (jnp.where(late, t, far), b))

    loop(2, late_block)

    @pl.when(two_back)
    def _():
        x_wrap(3 - NP).wait_recv()
        tiles(1, 1, 3, [EDGE])

    finalize(1, 1)
    send_out(1, 1)

    @pl.when(two_back)
    def _():
        x_plus(2).wait_recv()
        tiles(1, 0, 2, [EDGE, FULL])

    finalize(1, 0)
    send_out(1, 0)

    @pl.when(two_back)
    def _():
        for half in range(2):
            tiles(0, half, 2, [FULL, FULL])
        x_plus(1).wait_recv()
        tiles(0, 1, 1, [EDGE])

    finalize(0, 1)
    send_out(0, 1)

    @pl.when(two_back)
    def _():
        tiles(0, 0, 1, [FULL])
        x_plus(0).wait_recv()
        tiles(0, 0, 0, [EDGE])

    finalize(0, 0)
    send_out(0, 0)

    for half in range(2):
        for side in range(3):
            got(O, side, half)
        own_out(half).wait()
    for p in (K, V, Q, O):
        for side in range(3):
            for half in range(2):
                send(p, side, half).wait_send()

    @pl.when(x < 3)
    def _():
        for i in range(8):
            x_next(i).wait_send()

    @pl.when(relays_plus)
    def _():
        for i in range(NP):
            x_plus(i).wait_send()

    @pl.when(x < 2)
    def _():
        for i in range(NP, 8):
            x_minus(i).wait_send()

    @pl.when(relays_wrap)
    def _():
        for j in range(NM):
            x_wrap(j).wait_send()
        x_sink().wait_send()

    @pl.when(sid == 0)
    def _():
        for p in (K, V):
            for side in range(3):
                sink_out(p, side).wait_send()


def attend(lengths, q, k, v):
    bf = jnp.bfloat16
    dma = pltpu.SemaphoreType.DMA
    any_space = pl.BlockSpec(memory_space=pl.ANY)
    return pl.pallas_call(
        kernel,
        name="window_attention",
        out_shape=jax.ShapeDtypeStruct(q.shape, bf),
        in_specs=[pl.BlockSpec(memory_space=pltpu.SMEM), any_space, any_space, any_space],
        out_specs=any_space,
        scratch_shapes=[
            pltpu.VMEM((24, 2, HALF, DIM), bf),
            pltpu.VMEM((8, 2, HALF, DIM), bf),
            pltpu.VMEM((8, 2, HALF, DIM), bf),
            pltpu.VMEM((NM, 2, HALF, DIM), bf),
            pltpu.VMEM((2, 16, DIM), bf),
            *[pltpu.VMEM((SIDE, BLOCK, DIM), jnp.float32)] * 2,
            *[pltpu.VMEM((SIDE, BLOCK, 128), jnp.float32)] * 4,
            *[pltpu.VMEM((BLOCK, BLOCK), jnp.float32)] * 2,
            dma((4, 6)), dma((4, 6)),
            dma((8,)), dma((8,)),
            dma((NP,)), dma((NP,)),
            dma((NM,)), dma((NM,)),
            dma((NM,)), dma((NM,)),
            dma((1,)), dma((1,)),
            dma((2, 3)), dma((2,)),
            dma((10,)),
        ],
        compiler_params=pltpu.CompilerParams(
            collective_id=0, has_side_effects=True, vmem_limit_bytes=56 * 1024 * 1024
        ),
    )(lengths, q, k, v)


def shards(queries, key_heads, projected_value_heads, lengths):
    q, k, v = (z.transpose(1, 0, 2) for z in (queries, key_heads, projected_value_heads))
    return attend(lengths, q, k, v).transpose(1, 0, 2)


def solution(mesh):
    in_specs = (
        P(("batch", "seq"), None, None),
        P(("batch", "seq"), None, None),
        P(("batch", "seq"), None, None),
        P("batch"),
    )
    out_specs = P(("batch", "seq"), None, None)
    return jax.shard_map(shards, mesh=mesh, in_specs=in_specs, out_specs=out_specs, check_vma=False)
```

```python
import functools

import jax
import jax.numpy as jnp
from jax import lax
from jax.experimental import pallas as pl
from jax.experimental.pallas import tpu as pltpu
from jax.sharding import PartitionSpec as P

SINKS = 4
SIDE = 4
BLOCK = 512
HALF = 256
DIM = 256
NM = 5
NP = 8 - NM
C = 1.4426950408889634 / 16.0
NEG = -1e30
K, V, Q, O = 0, 1, 2, 3
FULL, DIAG, EDGE = 0, 1, 2


def kernel(
    len_ref, q_in, k_in, v_in, o_ref,
    kvb, qb, ob, rx, snk, acc0, acc1, mx0, mx1, ls0, ls1, sc0, sc1,
    ys, yr, xs, xr, ps, pr, ms, mr, ns, nr, ss, sr, ks, kr, loc,
):
    accs, mxs, lss, scs = (acc0, acc1), (mx0, mx1), (ls0, ls1), (sc0, sc1)
    sid = lax.axis_index("seq")
    x = lax.div(sid, SIDE)
    y = lax.rem(sid, SIDE)
    right = lax.rem(y + 1, SIDE)
    left = lax.rem(y + 3, SIDE)
    far = lax.rem(y + 2, SIDE)
    down = lax.rem(x + 1, SIDE)
    up = lax.rem(x + 3, SIDE)

    def dev(xx, yy):
        return {"seq": xx * SIDE + yy}

    def remote(src, dst, s, r, where):
        return pltpu.make_async_remote_copy(
            src_ref=src, dst_ref=dst, send_sem=s, recv_sem=r,
            device_id=where, device_id_type=pl.DeviceIdType.MESH,
        )

    def rows(half):
        return pl.ds(half * HALF, HALF)

    def src(p, n, half):
        if p == K:
            return k_in.at[n, rows(half)]
        if p == V:
            return v_in.at[n, rows(half)]
        if p == Q:
            return q_in.at[pl.ds(2 * n, 2), rows(half)]
        return ob.at[2 * n + half]

    def dst(p, n, half):
        if p in (K, V):
            return kvb.at[16 + 2 * n + half, p]
        if p == Q:
            return qb.at[2 * n + half]
        return o_ref.at[pl.ds(2 * n, 2), rows(half)]

    to = (right, left, far)
    come = (left, right, far)

    def send(p, side, half):
        k = 2 * side + half
        return remote(
            src(p, to[side], half), dst(p, y, half), ys.at[p, k], yr.at[p, k], dev(x, to[side])
        )

    def got(p, side, half):
        k = 2 * side + half
        d = dst(p, come[side], half)
        remote(d, d, ys.at[p, k], yr.at[p, k], dev(x, come[side])).wait_recv()

    def x_next(i):
        return remote(kvb.at[16 + i], kvb.at[8 + i], xs.at[i], xr.at[i], dev(down, y))

    def x_plus(i):
        return remote(kvb.at[8 + i], kvb.at[i], ps.at[i], pr.at[i], dev(down, y))

    def x_minus(i):
        return remote(kvb.at[16 + i], rx.at[i - NP], ms.at[i - NP], mr.at[i - NP], dev(up, y))

    def x_wrap(j):
        return remote(rx.at[j], kvb.at[NP + j], ns.at[j], nr.at[j], dev(up, y))

    def x_sink():
        return remote(snk, snk, ss.at[0], sr.at[0], dev(up, y))

    def sink_rows(p, n):
        return (k_in if p == K else v_in).at[n, pl.ds(0, 16)]

    def sink_out(p, side):
        n = to[side]
        return remote(sink_rows(p, n), snk.at[p], ks.at[p, side], kr.at[p], dev(x, n))

    def sink_own(p):
        return pltpu.make_async_copy(sink_rows(p, y), snk.at[p], loc.at[8 + p])

    def x_send(i):
        @pl.when(x < 3)
        def _():
            x_next(i).start()

        @pl.when((x < 2) & (i >= NP))
        def _():
            x_minus(i).start()

    relays_plus = (x == 1) | (x == 2)
    relays_wrap = (x == 0) | (x == 3)
    two_back = x >= 2

    lane = lax.broadcasted_iota(jnp.int32, (BLOCK, 128), 1)
    row = lax.rem(lax.broadcasted_iota(jnp.int32, (BLOCK, 128), 0), HALF)

    def scores(yq, half, k):
        q = qb[2 * yq + half].reshape(BLOCK, DIM)
        return lax.dot_general(
            q, k, (((1,), (1,)), ((), ())), preferred_element_type=jnp.float32
        )

    def update(yq, half, parts, v):
        acc, mx, ls = accs[half], mxs[half], lss[half]
        top = parts[0]
        for part in parts[1:]:
            top = jnp.maximum(top, part)
        old = mx[yq]
        new = jnp.maximum(old, jnp.max(top, axis=-1, keepdims=True))
        alpha = jnp.exp2((old - new) * C)
        weights = [jnp.exp2((part - new) * C) for part in parts]
        total = weights[0]
        for part in weights[1:]:
            total = total + part
        ls[yq] = ls[yq] * alpha + total
        mx[yq] = new
        rounded = jnp.concatenate([part.astype(jnp.bfloat16) for part in weights], axis=1)
        scale = jnp.concatenate([alpha, alpha], axis=1)
        acc[yq] = acc[yq] * scale + jnp.dot(rounded, v, preferred_element_type=jnp.float32)

    def cols(s):
        return [s[:, 128 * j : 128 * (j + 1)] for j in range(s.shape[1] // 128)]

    def keys_of(piece, n):
        return kvb[pl.ds(piece, n), 0].reshape(n * HALF, DIM)

    def values_of(piece, n):
        return kvb[pl.ds(piece, n), 1].reshape(n * HALF, DIM)

    def tiles(yq, half, piece, modes):
        n = len(modes)
        parts = cols(scores(yq, half, keys_of(piece, n)))
        for j in range(2 * n):
            key = lane + 128 * (j % 2)
            if modes[j // 2] == DIAG:
                parts[j] = jnp.where(key <= row, parts[j], NEG)
            if modes[j // 2] == EDGE:
                ok = key > row
                if half == 0 and j == 0:
                    ok = ok & (key >= jnp.where((x == 2) & (yq == 0), SINKS, 0))
                parts[j] = jnp.where(ok, parts[j], NEG)
        update(yq, half, parts, values_of(piece, n))

    def diag(yq):
        tiles(yq, 0, 16 + 2 * yq, [DIAG])
        tiles(yq, 1, 16 + 2 * yq, [FULL, DIAG])

    def edge(yq):
        tiles(yq, 0, 2 * yq, [EDGE, FULL])
        tiles(yq, 1, 2 * yq + 1, [EDGE])

    def loop(n, body):
        def step(t, carry):
            body(t)
            return carry

        lax.fori_loop(0, n, step, 0)

    def pipe(n, get):
        def qk(t, half):
            yq, b = get(t)
            scs[half][...] = scores(yq, half, keys_of(2 * b, 2))

        def softmax(t, half):
            yq, b = get(t)
            update(yq, half, cols(scs[half][...]), values_of(2 * b, 2))

        def step(t):
            qk(t, 1)
            softmax(t, 0)
            qk(jnp.minimum(t + 1, n - 1), 0)
            softmax(t, 1)

        @pl.when(n > 0)
        def _():
            qk(0, 0)
            loop(n, step)

    def sink_task(yq):
        pad = jnp.zeros((112, DIM), jnp.bfloat16)
        k = jnp.concatenate([snk[0], pad], axis=0)
        v = jnp.concatenate([snk[1], pad], axis=0)
        for half in range(2):
            update(yq, half, [jnp.where(lane < SINKS, scores(yq, half, k), NEG)], v)

    def finalize(yq, half):
        inv = 1.0 / jnp.sum(lss[half][yq], axis=-1, keepdims=True)
        ok = (x * SIDE + yq) * BLOCK + half * HALF + row < len_ref[0]
        ok = jnp.concatenate([ok, ok], axis=1)
        out = jnp.where(ok, accs[half][yq] * inv, 0.0)
        ob[2 * yq + half] = out.astype(jnp.bfloat16).reshape(2, HALF, DIM)

    def own_out(half):
        return pltpu.make_async_copy(ob.at[2 * y + half], dst(O, y, half), loc.at[half])

    def send_out(yq, half):
        @pl.when(y == yq)
        def _():
            own_out(half).start()

        for side in range(3):

            @pl.when(to[side] == yq)
            def _():
                send(O, side, half).start()

    barrier = pltpu.get_barrier_semaphore()
    for where in (dev(x, right), dev(x, left), dev(x, far), dev(down, y), dev(up, y)):
        pl.semaphore_signal(barrier, inc=1, device_id=where, device_id_type=pl.DeviceIdType.MESH)
    pl.semaphore_wait(barrier, 5)

    mine = [
        pltpu.make_async_copy(src(p, y, half), dst(p, y, half), loc.at[2 + 2 * p + half])
        for p in (K, V, Q)
        for half in range(2)
    ]

    @pl.when(sid == 0)
    def _():
        for p in (K, V):
            for side in range(3):
                sink_out(p, side).start()
            sink_own(p).start()

    for half in range(2):
        for side in range(2):
            send(K, side, half).start()
            send(V, side, half).start()
    for copy in mine:
        copy.start()
    for half in range(2):
        for side in range(2):
            send(Q, side, half).start()
    for half in range(2):
        send(K, 2, half).start()
        send(V, 2, half).start()
    for half in range(2):
        send(Q, 2, half).start()
    for half in range(2):
        mine[half].wait()
        mine[2 + half].wait()
        x_send(2 * y + half)

    @pl.when(sid == 0)
    def _():
        for p in (K, V):
            sink_own(p).wait()

    @pl.when((x == 0) & (y > 0))
    def _():
        for p in (K, V):
            remote(snk.at[p], snk.at[p], ks.at[p, 0], kr.at[p], dev(x, y)).wait_recv()

    @pl.when(x == 0)
    def _():
        x_sink().start()

    def init(t):
        for half in range(2):
            mxs[half][t] = jnp.full((BLOCK, 128), NEG, jnp.float32)
            lss[half][t] = jnp.zeros((BLOCK, 128), jnp.float32)
            accs[half][t] = jnp.zeros((BLOCK, DIM), jnp.float32)

    loop(SIDE, init)
    mine[4].wait()
    mine[5].wait()
    diag(y)
    for side in range(2):
        for half in range(2):
            got(K, side, half)
            got(V, side, half)
            x_send(2 * come[side] + half)

    def wrap(n):
        for half in range(2):
            i = 2 * n + half

            @pl.when(relays_wrap & (i >= NP))
            def _():
                x_minus(i).wait_recv()
                x_wrap(i - NP).start()

    lower = (left < y).astype(jnp.int32) + (right < y).astype(jnp.int32)

    @pl.when(x >= 1)
    def _():
        for half in range(2):
            x_next(2 * y + half).wait_recv()

    def own_tasks(t):
        return y, jnp.where(t < lower, 8 + jnp.where(t == 0, left, right), 4 + y)

    pipe(lower + (x >= 1).astype(jnp.int32), own_tasks)
    wrap(y)

    @pl.when(x == 3)
    def _():
        x_sink().wait_recv()
        x_sink().start()

    for half in range(2):
        for side in range(2):
            got(Q, side, half)

    def near(i):
        return i + (i >= far).astype(jnp.int32)

    loop(2, lambda t: diag(jnp.where(t == 0, left, right)))
    wrap(left)

    @pl.when(x >= 1)
    def _():
        for half in range(2):
            x_next(2 * left + half).wait_recv()

    pairs = 3 - lower
    start = ((y == 1) | (y == 2)).astype(jnp.int32)

    def near_tasks(t):
        own = t < pairs
        i = jnp.minimum(t + start, 2)
        r = t - pairs
        yq = jnp.where(
            own, near(jnp.minimum(i + 1, 2)), jnp.where(r == 0, left, jnp.where(r == 1, right, near(r - 2)))
        )
        b = jnp.where(own, 8 + near(i >> 1), 4 + jnp.where(r < 2, y, left))
        return yq, b

    pipe(pairs + jnp.where(x >= 1, 5, 0), near_tasks)

    wrap(right)
    for half in range(2):
        got(K, 2, half)
        got(V, 2, half)
        x_send(2 * far + half)

    @pl.when(x >= 1)
    def _():
        for half in range(2):
            x_next(2 * right + half).wait_recv()

    def right_tasks(t):
        t = t + jnp.where(x >= 1, 0, 3)
        yq = jnp.where(t < 3, near(t), near(far + t - 3))
        return yq, jnp.where(t < 3, 4 + right, 8 + far)

    pipe(jnp.where(x >= 1, 6, 3) - far, right_tasks)

    @pl.when(relays_plus)
    def _():
        @pl.when(far != 1)
        def _():
            x_plus(2).start()

        @pl.when(far >= 2)
        def _():
            x_plus(1).start()
            x_plus(0).start()


    def early(b):
        return (x == 2) & ((b == y) | (b == left))

    def wait_back(b):
        for half in range(2):
            x_wrap(2 * b + half - NP).wait_recv()

    @pl.when(two_back)
    def _():
        @pl.when(x == 2)
        def _():
            x_sink().wait_recv()

        loop(3, lambda t: sink_task(near(t)))

    def early_block(i):
        b = 3 - i

        @pl.when(early(b))
        def _():
            wait_back(b)
            edge(b)
            pipe(b - (far < b).astype(jnp.int32), lambda t: (near(t), b))

    loop(2, early_block)

    @pl.when(x >= 1)
    def _():
        for half in range(2):
            x_next(2 * far + half).wait_recv()

    @pl.when(relays_plus)
    def _():
        @pl.when(far == 1)
        def _():
            x_plus(2).start()

        @pl.when(far < 2)
        def _():
            x_plus(1).start()
            x_plus(0).start()

    wrap(far)
    for half in range(2):
        got(Q, 2, half)
    diag(far)

    def far_tasks(t):
        t = t + jnp.where(x >= 1, 0, 7)
        return jnp.where(t < 3, near(t), far), jnp.where(t < 3, 4 + far, t + 1)

    pipe(jnp.where(x >= 1, 7, 0) + far, far_tasks)

    pl.when(two_back)(lambda: sink_task(far))

    def late_block(i):
        b = 3 - i
        late = two_back & jnp.logical_not(early(b))

        @pl.when(late)
        def _():
            wait_back(b)
            edge(b)

        for half in range(2):
            finalize(b, half)
        for half in range(2):
            send_out(b, half)
        n = jnp.where(late, b, jnp.where(two_back & (far < b), 1, 0))
        pipe(n, lambda t: (jnp.where(late, t, far), b))

    loop(2, late_block)

    @pl.when(two_back)
    def _():
        x_wrap(3 - NP).wait_recv()
        tiles(1, 1, 3, [EDGE])

    finalize(1, 1)
    send_out(1, 1)

    @pl.when(two_back)
    def _():
        x_plus(2).wait_recv()
        tiles(1, 0, 2, [EDGE, FULL])

    finalize(1, 0)
    send_out(1, 0)

    @pl.when(two_back)
    def _():
        for half in range(2):
            tiles(0, half, 2, [FULL, FULL])
        x_plus(1).wait_recv()
        tiles(0, 1, 1, [EDGE])

    finalize(0, 1)
    send_out(0, 1)

    @pl.when(two_back)
    def _():
        tiles(0, 0, 1, [FULL])
        x_plus(0).wait_recv()
        tiles(0, 0, 0, [EDGE])

    finalize(0, 0)
    send_out(0, 0)

    for half in range(2):
        for side in range(3):
            got(O, side, half)
        own_out(half).wait()
    for p in (K, V, Q, O):
        for side in range(3):
            for half in range(2):
                send(p, side, half).wait_send()

    @pl.when(x < 3)
    def _():
        for i in range(8):
            x_next(i).wait_send()

    @pl.when(relays_plus)
    def _():
        for i in range(NP):
            x_plus(i).wait_send()

    @pl.when(x < 2)
    def _():
        for i in range(NP, 8):
            x_minus(i).wait_send()

    @pl.when(relays_wrap)
    def _():
        for j in range(NM):
            x_wrap(j).wait_send()
        x_sink().wait_send()

    @pl.when(sid == 0)
    def _():
        for p in (K, V):
            for side in range(3):
                sink_out(p, side).wait_send()


def attend(lengths, q, k, v):
    bf = jnp.bfloat16
    dma = pltpu.SemaphoreType.DMA
    any_space = pl.BlockSpec(memory_space=pl.ANY)
    return pl.pallas_call(
        kernel,
        name="window_attention",
        out_shape=jax.ShapeDtypeStruct(q.shape, bf),
        in_specs=[pl.BlockSpec(memory_space=pltpu.SMEM), any_space, any_space, any_space],
        out_specs=any_space,
        scratch_shapes=[
            pltpu.VMEM((24, 2, HALF, DIM), bf),
            pltpu.VMEM((8, 2, HALF, DIM), bf),
            pltpu.VMEM((8, 2, HALF, DIM), bf),
            pltpu.VMEM((NM, 2, HALF, DIM), bf),
            pltpu.VMEM((2, 16, DIM), bf),
            *[pltpu.VMEM((SIDE, BLOCK, DIM), jnp.float32)] * 2,
            *[pltpu.VMEM((SIDE, BLOCK, 128), jnp.float32)] * 4,
            *[pltpu.VMEM((BLOCK, BLOCK), jnp.float32)] * 2,
            dma((4, 6)), dma((4, 6)),
            dma((8,)), dma((8,)),
            dma((NP,)), dma((NP,)),
            dma((NM,)), dma((NM,)),
            dma((NM,)), dma((NM,)),
            dma((1,)), dma((1,)),
            dma((2, 3)), dma((2,)),
            dma((10,)),
        ],
        compiler_params=pltpu.CompilerParams(
            collective_id=0, has_side_effects=True, vmem_limit_bytes=34 * 1024 * 1024
        ),
    )(lengths, q, k, v)


def shards(queries, key_heads, projected_value_heads, lengths):
    q, k, v = (z.transpose(1, 0, 2) for z in (queries, key_heads, projected_value_heads))
    return attend(lengths, q, k, v).transpose(1, 0, 2)


def solution(mesh):
    in_specs = (
        P(("batch", "seq"), None, None),
        P(("batch", "seq"), None, None),
        P(("batch", "seq"), None, None),
        P("batch"),
    )
    out_specs = P(("batch", "seq"), None, None)
    return jax.shard_map(shards, mesh=mesh, in_specs=in_specs, out_specs=out_specs, check_vma=False)
```

```python
import functools

import jax
import jax.numpy as jnp
from jax import lax
from jax.experimental import pallas as pl
from jax.experimental.pallas import tpu as pltpu
from jax.sharding import PartitionSpec as P

SINKS = 4
SIDE = 4
BLOCK = 512
HALF = 256
DIM = 256
NM = 5
NP = 8 - NM
C = 1.4426950408889634 / 16.0
NEG = -1e30
K, V, Q, O = 0, 1, 2, 3
FULL, DIAG, EDGE = 0, 1, 2


def kernel(
    len_ref, q_in, k_in, v_in, o_ref,
    kvb, qb, ob, rx, snk, acc0, acc1, mx0, mx1, ls0, ls1, sc0, sc1,
    ys, yr, xs, xr, ps, pr, ms, mr, ns, nr, ss, sr, ks, kr, loc,
):
    accs, mxs, lss, scs = (acc0, acc1), (mx0, mx1), (ls0, ls1), (sc0, sc1)
    sid = lax.axis_index("seq")
    x = lax.div(sid, SIDE)
    y = lax.rem(sid, SIDE)
    right = lax.rem(y + 1, SIDE)
    left = lax.rem(y + 3, SIDE)
    far = lax.rem(y + 2, SIDE)
    down = lax.rem(x + 1, SIDE)
    up = lax.rem(x + 3, SIDE)

    def dev(xx, yy):
        return {"seq": xx * SIDE + yy}

    def remote(src, dst, s, r, where):
        return pltpu.make_async_remote_copy(
            src_ref=src, dst_ref=dst, send_sem=s, recv_sem=r,
            device_id=where, device_id_type=pl.DeviceIdType.MESH,
        )

    def rows(half):
        return pl.ds(half * HALF, HALF)

    def src(p, n, half):
        if p == K:
            return k_in.at[n, rows(half)]
        if p == V:
            return v_in.at[n, rows(half)]
        if p == Q:
            return q_in.at[pl.ds(2 * n, 2), rows(half)]
        return ob.at[2 * n + half]

    def dst(p, n, half):
        if p in (K, V):
            return kvb.at[16 + 2 * n + half, p]
        if p == Q:
            return qb.at[2 * n + half]
        return o_ref.at[pl.ds(2 * n, 2), rows(half)]

    to = (right, left, far)
    come = (left, right, far)

    def send(p, side, half):
        k = 2 * side + half
        return remote(
            src(p, to[side], half), dst(p, y, half), ys.at[p, k], yr.at[p, k], dev(x, to[side])
        )

    def got(p, side, half):
        k = 2 * side + half
        d = dst(p, come[side], half)
        remote(d, d, ys.at[p, k], yr.at[p, k], dev(x, come[side])).wait_recv()

    def x_next(i):
        return remote(kvb.at[16 + i], kvb.at[8 + i], xs.at[i], xr.at[i], dev(down, y))

    def x_plus(i):
        return remote(kvb.at[8 + i], kvb.at[i], ps.at[i], pr.at[i], dev(down, y))

    def x_minus(i):
        return remote(kvb.at[16 + i], rx.at[i - NP], ms.at[i - NP], mr.at[i - NP], dev(up, y))

    def x_wrap(j):
        return remote(rx.at[j], kvb.at[NP + j], ns.at[j], nr.at[j], dev(up, y))

    def x_sink():
        return remote(snk, snk, ss.at[0], sr.at[0], dev(up, y))

    def sink_rows(p, n):
        return (k_in if p == K else v_in).at[n, pl.ds(0, 16)]

    def sink_out(p, side):
        n = to[side]
        return remote(sink_rows(p, n), snk.at[p], ks.at[p, side], kr.at[p], dev(x, n))

    def sink_own(p):
        return pltpu.make_async_copy(sink_rows(p, y), snk.at[p], loc.at[8 + p])

    def x_send(i):
        @pl.when(x < 3)
        def _():
            x_next(i).start()

        @pl.when((x < 2) & (i >= NP))
        def _():
            x_minus(i).start()

    relays_plus = (x == 1) | (x == 2)
    relays_wrap = (x == 0) | (x == 3)
    two_back = x >= 2

    lane = lax.broadcasted_iota(jnp.int32, (BLOCK, 128), 1)
    row = lax.rem(lax.broadcasted_iota(jnp.int32, (BLOCK, 128), 0), HALF)

    def scores(yq, half, k):
        q = qb[2 * yq + half].reshape(BLOCK, DIM)
        return lax.dot_general(
            q, k, (((1,), (1,)), ((), ())), preferred_element_type=jnp.float32
        )

    def update(yq, half, parts, v):
        acc, mx, ls = accs[half], mxs[half], lss[half]
        top = parts[0]
        for part in parts[1:]:
            top = jnp.maximum(top, part)
        old = mx[yq]
        new = jnp.maximum(old, jnp.max(top, axis=-1, keepdims=True))
        alpha = jnp.exp2((old - new) * C)
        weights = [jnp.exp2((part - new) * C) for part in parts]
        total = weights[0]
        for part in weights[1:]:
            total = total + part
        ls[yq] = ls[yq] * alpha + total
        mx[yq] = new
        rounded = jnp.concatenate([part.astype(jnp.bfloat16) for part in weights], axis=1)
        scale = jnp.concatenate([alpha, alpha], axis=1)
        acc[yq] = acc[yq] * scale + jnp.dot(rounded, v, preferred_element_type=jnp.float32)

    def cols(s):
        return [s[:, 128 * j : 128 * (j + 1)] for j in range(s.shape[1] // 128)]

    def keys_of(piece, n):
        return kvb[pl.ds(piece, n), 0].reshape(n * HALF, DIM)

    def values_of(piece, n):
        return kvb[pl.ds(piece, n), 1].reshape(n * HALF, DIM)

    def tiles(yq, half, piece, modes):
        n = len(modes)
        parts = cols(scores(yq, half, keys_of(piece, n)))
        for j in range(2 * n):
            key = lane + 128 * (j % 2)
            if modes[j // 2] == DIAG:
                parts[j] = jnp.where(key <= row, parts[j], NEG)
            if modes[j // 2] == EDGE:
                ok = key > row
                if half == 0 and j == 0:
                    ok = ok & (key >= jnp.where((x == 2) & (yq == 0), SINKS, 0))
                parts[j] = jnp.where(ok, parts[j], NEG)
        update(yq, half, parts, values_of(piece, n))

    def diag(yq):
        tiles(yq, 0, 16 + 2 * yq, [DIAG])
        tiles(yq, 1, 16 + 2 * yq, [FULL, DIAG])

    def edge(yq):
        tiles(yq, 0, 2 * yq, [EDGE, FULL])
        tiles(yq, 1, 2 * yq + 1, [EDGE])

    def loop(n, body):
        def step(t, carry):
            body(t)
            return carry

        lax.fori_loop(0, n, step, 0)

    def pipe(n, get):
        def qk(t, half):
            yq, b = get(t)
            scs[half][...] = scores(yq, half, keys_of(2 * b, 2))

        def softmax(t, half):
            yq, b = get(t)
            update(yq, half, cols(scs[half][...]), values_of(2 * b, 2))

        def step(t):
            qk(t, 1)
            softmax(t, 0)
            qk(jnp.minimum(t + 1, n - 1), 0)
            softmax(t, 1)

        @pl.when(n > 0)
        def _():
            qk(0, 0)
            loop(n, step)

    def sink_task(yq):
        pad = jnp.zeros((112, DIM), jnp.bfloat16)
        k = jnp.concatenate([snk[0], pad], axis=0)
        v = jnp.concatenate([snk[1], pad], axis=0)
        for half in range(2):
            update(yq, half, [jnp.where(lane < SINKS, scores(yq, half, k), NEG)], v)

    def finalize(yq, half):
        inv = 1.0 / jnp.sum(lss[half][yq], axis=-1, keepdims=True)
        ok = (x * SIDE + yq) * BLOCK + half * HALF + row < len_ref[0]
        ok = jnp.concatenate([ok, ok], axis=1)
        out = jnp.where(ok, accs[half][yq] * inv, 0.0)
        ob[2 * yq + half] = out.astype(jnp.bfloat16).reshape(2, HALF, DIM)

    def own_out(half):
        return pltpu.make_async_copy(ob.at[2 * y + half], dst(O, y, half), loc.at[half])

    def send_out(yq, half):
        @pl.when(y == yq)
        def _():
            own_out(half).start()

        for side in range(3):

            @pl.when(to[side] == yq)
            def _():
                send(O, side, half).start()

    barrier = pltpu.get_barrier_semaphore()
    for where in (dev(x, right), dev(x, left), dev(x, far), dev(down, y), dev(up, y)):
        pl.semaphore_signal(barrier, inc=1, device_id=where, device_id_type=pl.DeviceIdType.MESH)
    pl.semaphore_wait(barrier, 5)

    mine = [
        pltpu.make_async_copy(src(p, y, half), dst(p, y, half), loc.at[2 + 2 * p + half])
        for p in (K, V, Q)
        for half in range(2)
    ]

    @pl.when(sid == 0)
    def _():
        for p in (K, V):
            for side in range(3):
                sink_out(p, side).start()
            sink_own(p).start()

    for half in range(2):
        for side in range(2):
            send(K, side, half).start()
            send(V, side, half).start()
    for copy in mine:
        copy.start()
    for half in range(2):
        for side in range(2):
            send(Q, side, half).start()
    for half in range(2):
        send(K, 2, half).start()
        send(V, 2, half).start()
    for half in range(2):
        send(Q, 2, half).start()
    for half in range(2):
        mine[half].wait()
        mine[2 + half].wait()
        x_send(2 * y + half)

    @pl.when(sid == 0)
    def _():
        for p in (K, V):
            sink_own(p).wait()

    @pl.when((x == 0) & (y > 0))
    def _():
        for p in (K, V):
            remote(snk.at[p], snk.at[p], ks.at[p, 0], kr.at[p], dev(x, y)).wait_recv()

    @pl.when(x == 0)
    def _():
        x_sink().start()

    def init(t):
        for half in range(2):
            mxs[half][t] = jnp.full((BLOCK, 128), NEG, jnp.float32)
            lss[half][t] = jnp.zeros((BLOCK, 128), jnp.float32)
            accs[half][t] = jnp.zeros((BLOCK, DIM), jnp.float32)

    loop(SIDE, init)
    mine[4].wait()
    mine[5].wait()
    diag(y)
    for side in range(2):
        for half in range(2):
            got(K, side, half)
            got(V, side, half)
            x_send(2 * come[side] + half)

    def wrap(n):
        for half in range(2):
            i = 2 * n + half

            @pl.when(relays_wrap & (i >= NP))
            def _():
                x_minus(i).wait_recv()
                x_wrap(i - NP).start()

    lower = (left < y).astype(jnp.int32) + (right < y).astype(jnp.int32)

    @pl.when(x >= 1)
    def _():
        for half in range(2):
            x_next(2 * y + half).wait_recv()

    def own_tasks(t):
        return y, jnp.where(t < lower, 8 + jnp.where(t == 0, left, right), 4 + y)

    pipe(lower + (x >= 1).astype(jnp.int32), own_tasks)
    wrap(y)

    @pl.when(x == 3)
    def _():
        x_sink().wait_recv()
        x_sink().start()

    for half in range(2):
        for side in range(2):
            got(Q, side, half)

    def near(i):
        return i + (i >= far).astype(jnp.int32)

    loop(2, lambda t: diag(jnp.where(t == 0, left, right)))
    wrap(left)

    @pl.when(x >= 1)
    def _():
        for half in range(2):
            x_next(2 * left + half).wait_recv()

    pairs = 3 - lower
    start = ((y == 1) | (y == 2)).astype(jnp.int32)

    def near_tasks(t):
        own = t < pairs
        i = jnp.minimum(t + start, 2)
        r = t - pairs
        yq = jnp.where(
            own, near(jnp.minimum(i + 1, 2)), jnp.where(r == 0, left, jnp.where(r == 1, right, near(r - 2)))
        )
        b = jnp.where(own, 8 + near(i >> 1), 4 + jnp.where(r < 2, y, left))
        return yq, b

    pipe(pairs + jnp.where(x >= 1, 5, 0), near_tasks)

    wrap(right)
    for half in range(2):
        got(K, 2, half)
        got(V, 2, half)
        x_send(2 * far + half)

    @pl.when(x >= 1)
    def _():
        for half in range(2):
            x_next(2 * right + half).wait_recv()

    def right_tasks(t):
        t = t + jnp.where(x >= 1, 0, 3)
        yq = jnp.where(t < 3, near(t), near(far + t - 3))
        return yq, jnp.where(t < 3, 4 + right, 8 + far)

    pipe(jnp.where(x >= 1, 6, 3) - far, right_tasks)

    @pl.when(relays_plus)
    def _():
        @pl.when(far != 1)
        def _():
            x_plus(2).start()

        @pl.when(far >= 2)
        def _():
            x_plus(1).start()
            x_plus(0).start()


    def early(b):
        return (x == 2) & ((b == y) | (b == left))

    def wait_back(b):
        for half in range(2):
            x_wrap(2 * b + half - NP).wait_recv()

    @pl.when(two_back)
    def _():
        @pl.when(x == 2)
        def _():
            x_sink().wait_recv()

        loop(3, lambda t: sink_task(near(t)))

    def early_block(i):
        b = 3 - i

        @pl.when(early(b))
        def _():
            wait_back(b)
            edge(b)
            pipe(b - (far < b).astype(jnp.int32), lambda t: (near(t), b))

    loop(2, early_block)

    @pl.when(x >= 1)
    def _():
        for half in range(2):
            x_next(2 * far + half).wait_recv()

    @pl.when(relays_plus)
    def _():
        @pl.when(far == 1)
        def _():
            x_plus(2).start()

        @pl.when(far < 2)
        def _():
            x_plus(1).start()
            x_plus(0).start()

    pl.when(x == 0)(lambda: wrap(far))
    for half in range(2):
        got(Q, 2, half)
    diag(far)

    def far_tasks(t):
        t = t + jnp.where(x >= 1, 0, 7)
        return jnp.where(t < 3, near(t), far), jnp.where(t < 3, 4 + far, t + 1)

    pipe(jnp.where(x >= 1, 7, 0) + far, far_tasks)
    pl.when(x == 3)(lambda: wrap(far))

    pl.when(two_back)(lambda: sink_task(far))

    def late_block(i):
        b = 3 - i
        late = two_back & jnp.logical_not(early(b))

        @pl.when(late)
        def _():
            wait_back(b)
            edge(b)

        for half in range(2):
            finalize(b, half)
        for half in range(2):
            send_out(b, half)
        n = jnp.where(late, b, jnp.where(two_back & (far < b), 1, 0))
        pipe(n, lambda t: (jnp.where(late, t, far), b))

    loop(2, late_block)

    @pl.when(two_back)
    def _():
        x_wrap(3 - NP).wait_recv()
        tiles(1, 1, 3, [EDGE])

    finalize(1, 1)
    send_out(1, 1)

    @pl.when(two_back)
    def _():
        x_plus(2).wait_recv()
        tiles(1, 0, 2, [EDGE, FULL])

    finalize(1, 0)
    send_out(1, 0)

    @pl.when(two_back)
    def _():
        for half in range(2):
            tiles(0, half, 2, [FULL, FULL])
        x_plus(1).wait_recv()
        tiles(0, 1, 1, [EDGE])

    finalize(0, 1)
    send_out(0, 1)

    @pl.when(two_back)
    def _():
        tiles(0, 0, 1, [FULL])
        x_plus(0).wait_recv()
        tiles(0, 0, 0, [EDGE])

    finalize(0, 0)
    send_out(0, 0)

    for half in range(2):
        for side in range(3):
            got(O, side, half)
        own_out(half).wait()
    for p in (K, V, Q, O):
        for side in range(3):
            for half in range(2):
                send(p, side, half).wait_send()

    @pl.when(x < 3)
    def _():
        for i in range(8):
            x_next(i).wait_send()

    @pl.when(relays_plus)
    def _():
        for i in range(NP):
            x_plus(i).wait_send()

    @pl.when(x < 2)
    def _():
        for i in range(NP, 8):
            x_minus(i).wait_send()

    @pl.when(relays_wrap)
    def _():
        for j in range(NM):
            x_wrap(j).wait_send()
        x_sink().wait_send()

    @pl.when(sid == 0)
    def _():
        for p in (K, V):
            for side in range(3):
                sink_out(p, side).wait_send()


def attend(lengths, q, k, v):
    bf = jnp.bfloat16
    dma = pltpu.SemaphoreType.DMA
    any_space = pl.BlockSpec(memory_space=pl.ANY)
    return pl.pallas_call(
        kernel,
        name="window_attention",
        out_shape=jax.ShapeDtypeStruct(q.shape, bf),
        in_specs=[pl.BlockSpec(memory_space=pltpu.SMEM), any_space, any_space, any_space],
        out_specs=any_space,
        scratch_shapes=[
            pltpu.VMEM((24, 2, HALF, DIM), bf),
            pltpu.VMEM((8, 2, HALF, DIM), bf),
            pltpu.VMEM((8, 2, HALF, DIM), bf),
            pltpu.VMEM((NM, 2, HALF, DIM), bf),
            pltpu.VMEM((2, 16, DIM), bf),
            *[pltpu.VMEM((SIDE, BLOCK, DIM), jnp.float32)] * 2,
            *[pltpu.VMEM((SIDE, BLOCK, 128), jnp.float32)] * 4,
            *[pltpu.VMEM((BLOCK, BLOCK), jnp.float32)] * 2,
            dma((4, 6)), dma((4, 6)),
            dma((8,)), dma((8,)),
            dma((NP,)), dma((NP,)),
            dma((NM,)), dma((NM,)),
            dma((NM,)), dma((NM,)),
            dma((1,)), dma((1,)),
            dma((2, 3)), dma((2,)),
            dma((10,)),
        ],
        compiler_params=pltpu.CompilerParams(
            collective_id=0, has_side_effects=True, vmem_limit_bytes=34 * 1024 * 1024
        ),
    )(lengths, q, k, v)


def shards(queries, key_heads, projected_value_heads, lengths):
    q, k, v = (z.transpose(1, 0, 2) for z in (queries, key_heads, projected_value_heads))
    return attend(lengths, q, k, v).transpose(1, 0, 2)


def solution(mesh):
    in_specs = (
        P(("batch", "seq"), None, None),
        P(("batch", "seq"), None, None),
        P(("batch", "seq"), None, None),
        P("batch"),
    )
    out_specs = P(("batch", "seq"), None, None)
    return jax.shard_map(shards, mesh=mesh, in_specs=in_specs, out_specs=out_specs, check_vma=False)
```
